32 devices in a mesh: dp: 8 (over z, x), tensor: 4 (over y, core).
Axes of the slice: x: 2, y: 2, z: 4, core: 2. Of those that a mesh axis runs over, the one named last changes fastest.
Arguments:
- tokens: bfloat16 [2048, 8192], P('dp', 'tensor'), may hold values from -6 to 6
- block_routing: int32 [8, 2], replicated, may hold values from -1 to 7, as said below
- frozen_up_weight: bfloat16 [8192, 28672], P('tensor', 'dp'), may hold values from -0.0625 to 0.0625
- adapter_down_weight: bfloat16 [32, 8192], P(None, 'tensor'), may hold values from -0.0625 to 0.0625
- adapter_up_weight: bfloat16 [32, 28672], P(None, 'dp'), may hold values from -6 to 6
- magnitude: float32 [28672], P('dp'), may hold values from 0.5 to 2
- cotangent: bfloat16 [1024, 28672], P('tensor', 'dp'), may hold values from -6 to 6
Outputs:
- projected: bfloat16 [1024, 28672], P('tensor', 'dp')
- grad_a: float32 [32, 8192], P(None, 'tensor')
- grad_b: float32 [32, 28672], P(None, 'dp')
- grad_m: float32 [28672], P('dp')
The draws below stay inside these ranges and needn't reach their ends.
Inputs may be any that keep to these rules, and one draw needn't show every extreme that they name: `block_routing`: row d lists where the two blocks of dp index d go. Live blocks come first and -1 marks a padding block. A first live block stays on its own index; a second live block goes to index (d + half the dp size) mod the dp size, which then has no live block. Every dp index receives exactly one block. In every draw some index has two live blocks and some has none.
All inputs are finite; a program needn't handle non-finite values.
Results may differ from the reference program's by a relative error of at most 0.018.
Values may be sent and summed in bfloat16 or wider, within the bound.
A program may use at most 128 MiB of HBM per device.

```python
import math
import jax
import jax.numpy as jnp
from jax import lax

MODEL_WIDTH = 8192
HIDDEN_UNITS = 28672
ADAPTER_RANK = 32
SLOTS = 2
BLK = 128
T_LIVE = 1024
N_DP = 8
N_TENSOR = 4


def draw_block_routing(key, part):
    half_count = N_DP // 2
    key_kind, key_pick, key_force = jax.random.split(key, 3)
    kinds = jax.random.randint(key_kind, (half_count,), 0, 3)
    chosen = jax.random.randint(key_pick, (), 0, half_count)
    forced = 1 + jax.random.randint(key_force, (), 0, 2)
    kinds = jnp.where(jnp.arange(half_count) == chosen, forced, kinds)
    lower_counts = jnp.where(kinds == 0, 1, jnp.where(kinds == 1, 2, 0))
    counts = jnp.concatenate([lower_counts, 2 - lower_counts])
    devices = jnp.arange(N_DP, dtype=jnp.int32)
    partner = (devices + half_count) % N_DP
    first_slot = jnp.where(counts >= 1, devices, -1)
    second_slot = jnp.where(counts == 2, partner, -1)
    return jnp.stack([first_slot, second_slot], axis=1).astype(jnp.int32)


def level_of(stream_key, shape, cuts, least, high):
    def one(position, parts):
        steps = jax.random.uniform(jax.random.fold_in(jax.random.fold_in(stream_key, 6), position), (parts,), jnp.float32, least / len(cuts), high / len(cuts))
        return jnp.repeat(jnp.exp(steps), shape[position] // parts).reshape((-1,) + (1,) * (len(shape) - position - 1))

    level = one(*cuts[0])
    for cut in cuts[1:]:
        level = level * one(*cut)
    return level


def scatter_about(stream_key, shape, deviation, most, cuts=(), kind=jnp.bfloat16):
    loudness = level_of(stream_key, shape, cuts, -0.22, 0.18) if cuts else 1.0
    result = jax.random.normal(stream_key, shape, jnp.float32) * deviation * loudness
    return jnp.minimum(jnp.maximum(result, -most), most).astype(kind)


def setup_inputs(seed: int = 0) -> dict:
    keys = jax.random.split(jax.random.key(seed), 8)
    return {
        "tokens": scatter_about(keys[0], (N_DP * SLOTS * BLK, MODEL_WIDTH), 1.0, 6.0, ((0, 8), (1, 4))),
        "block_routing": draw_block_routing(jax.random.fold_in(keys[7], 71), 0),
        "frozen_up_weight": scatter_about(keys[2], (MODEL_WIDTH, HIDDEN_UNITS), MODEL_WIDTH ** -0.5, 0.0625, ((0, 4), (1, 8))),
        "adapter_down_weight": scatter_about(keys[3], (ADAPTER_RANK, MODEL_WIDTH), MODEL_WIDTH ** -0.5, 0.0625, ((1, 4),)),
        "adapter_up_weight": scatter_about(keys[4], (ADAPTER_RANK, HIDDEN_UNITS), 1.0, 6.0, ((1, 8),)),
        "magnitude": jnp.clip(jnp.exp(math.log(2.0) - 1.3862944 * jax.random.uniform(keys[5], (HIDDEN_UNITS,), jnp.float32) ** level_of(keys[5], (HIDDEN_UNITS,), ((0, 8),), -0.2, 0.2)), 0.5, 2.0),
        "cotangent": scatter_about(keys[6], (T_LIVE, HIDDEN_UNITS), 1.0, 6.0, ((0, 4), (1, 8))),
    }


def contract_dims(left, right, left_dim, right_dim):
    return lax.dot_general(left, right, (((left_dim,), (right_dim,)), ((), ())), preferred_element_type=jnp.float32)

def reference(tokens, block_routing, frozen_up_weight, adapter_down_weight, adapter_up_weight, magnitude, cotangent):
    adapter_scale = 1.0 / math.sqrt(ADAPTER_RANK)
    flat_plan = block_routing.reshape(-1)
    matches = (flat_plan[None, :] == jnp.arange(N_DP, dtype=jnp.int32)[:, None]).astype(jnp.int32)
    source = lax.optimization_barrier(jnp.sum(matches * jnp.arange(N_DP * SLOTS, dtype=jnp.int32)[None, :], axis=1)).astype(jnp.int32)
    blocks = tokens.reshape(N_DP * SLOTS, BLK, MODEL_WIDTH)
    active_tokens = jnp.take(blocks, source, axis=0).reshape(T_LIVE, MODEL_WIDTH)
    group_width = MODEL_WIDTH // N_TENSOR
    frozen_sum = jnp.zeros((T_LIVE, HIDDEN_UNITS), jnp.float32)
    for group_idx in range(N_TENSOR):
        lower = group_idx * group_width
        partial_prod = jnp.dot(active_tokens[:, lower:lower + group_width], frozen_up_weight[lower:lower + group_width, :], preferred_element_type=jnp.float32)
        rounded = lax.optimization_barrier(partial_prod.astype(jnp.bfloat16))
        frozen_sum = frozen_sum + rounded.astype(jnp.float32)
    down_factor_half = contract_dims(active_tokens, adapter_down_weight, 1, 1).astype(jnp.bfloat16)
    column_span = HIDDEN_UNITS // N_DP

    def column_squares(block_position):
        weight_columns = lax.dynamic_slice_in_dim(frozen_up_weight, block_position * column_span, column_span, 1).astype(jnp.float32)
        up_factor_columns = lax.dynamic_slice_in_dim(adapter_up_weight, block_position * column_span, column_span, 1)
        merged_weight = weight_columns + adapter_scale * contract_dims(adapter_down_weight, up_factor_columns, 0, 0)
        return lax.optimization_barrier(jnp.sum(merged_weight * merged_weight, axis=0))
    col_square = lax.map(column_squares, jnp.arange(N_DP, dtype=jnp.int32)).reshape(HIDDEN_UNITS)
    col_norm = jnp.maximum(jnp.sqrt(col_square), 0.5)
    unscaled_output = frozen_sum + adapter_scale * jnp.dot(down_factor_half, adapter_up_weight, preferred_element_type=jnp.float32)
    col_factor = magnitude / col_norm
    projected = (unscaled_output * col_factor).astype(jnp.bfloat16)
    inverse = 1.0 / math.sqrt(T_LIVE)
    cot_full = cotangent.astype(jnp.float32)
    scaled_gradient = (cot_full * col_factor * inverse).astype(jnp.bfloat16)
    grad_m = lax.optimization_barrier(jnp.sum(cot_full * unscaled_output, axis=0)) / col_norm * inverse
    grad_b = adapter_scale * contract_dims(down_factor_half, scaled_gradient, 0, 0)
    row_gradient = contract_dims(scaled_gradient, adapter_up_weight, 1, 1).astype(jnp.bfloat16)
    grad_a = adapter_scale * contract_dims(row_gradient, active_tokens, 0, 0)
    return (projected, grad_a, grad_b, grad_m)
```

```python
import functools
import math

import jax
import jax.numpy as jnp
from jax import lax
from jax.experimental import pallas as pl
from jax.experimental.pallas import tpu as pltpu
from jax.sharding import PartitionSpec as P

BLK = 128
ROWS = 16
CHUNKS = BLK // ROWS
HALVES = 2
UNITS = CHUNKS * HALVES
AHEAD = 2
LAG = 2
EARLY = 3
LANES = 128
MESH = pl.DeviceIdType.MESH
F32 = jnp.float32
BF16 = jnp.bfloat16


def mirrored(value, bits):
    result = 0
    for position in range(bits):
        result = result + (value // (1 << position)) % 2 * (1 << (bits - 1 - position))
    return result


def flipped(value, bit):
    return value + bit - 2 * bit * ((value // bit) % 2)


def dots(left, right, left_dim, right_dim):
    return lax.dot_general(
        left, right, (((left_dim,), (right_dim,)), ((), ())), preferred_element_type=F32
    )


def kernel(
    cfg,
    tok_hbm, routing, w_hbm, down_hbm, up_hbm, mag_hbm, cot_hbm,
    out, ga_out, gb_out, gm_out,
    tok_in, down, up, mag, cot, w,
    raw, tok, part, near, pair, far, sq, sq_near, sq_far, factor, norm, sg,
    rp, rp_in, rgt, rg, rg_turned, proj_down, proj_turned, gm_acc,
    gb_part, gb_near, gb_sum, gb_far, gb_all, gm_in, d_loc, d_in, d_all,
    in_sem, w_sem, s0_send, s0_recv, st_send, st_recv, nr_send, nr_recv, fr_send, fr_recv,
    ms_send, ms_recv, ds_send, ds_recv, db_send, db_recv, gm_send, gm_recv,
):
    dp, tp, width, cols, rank, tile = cfg
    bits = dp.bit_length() - 1
    per = dp // tp
    tiles = cols // tile
    cut = (tiles + 1) // 2
    pieces = ((0, cut), (cut, tiles))
    order = [mirrored(g, per.bit_length() - 1) for g in range(per)]
    scale = 1.0 / math.sqrt(rank)
    inverse = 1.0 / math.sqrt(dp * BLK)
    high = per * ROWS
    d = lax.axis_index("dp")
    t = lax.axis_index("tensor")
    core = t % 2
    side = t // 2
    t_near, t_far = flipped(t, 1), flipped(t, 2)
    hops = [flipped(d, dp >> (k + 1)) for k in range(bits)]
    homes = (d // per, hops[0] // per)

    def copy(src, dst, send, recv, target):
        return pltpu.make_async_remote_copy(
            src_ref=src, dst_ref=dst, send_sem=send, recv_sem=recv,
            device_id=target, device_id_type=MESH,
        )

    def when(condition, action):
        pl.when(condition)(action)

    def to_dp(k):
        return {"dp": hops[k]}

    near_id, far_id = {"tensor": t_near}, {"tensor": t_far}

    def span(p):
        return pl.ds(pieces[p][0] * tile, (pieces[p][1] - pieces[p][0]) * tile)

    def tile_at(n):
        if isinstance(n, int):
            return pl.ds(n * tile, tile)
        return pl.ds(pl.multiple_of(n * tile, tile), tile)

    def w_copy(n):
        return pltpu.make_async_copy(w_hbm.at[:, tile_at(n)], w.at[:, tile_at(n)], w_sem.at[n])

    tok_copy = pltpu.make_async_copy(tok_hbm, tok_in, in_sem.at[0])
    loads = [
        pltpu.make_async_copy(down_hbm, down, in_sem.at[1]),
        pltpu.make_async_copy(up_hbm, up, in_sem.at[2]),
        pltpu.make_async_copy(mag_hbm, mag, in_sem.at[3]),
    ]
    cot_loads = [
        pltpu.make_async_copy(cot_hbm.at[g], cot.at[order[g]], in_sem.at[4 + g])
        for g in range(per)
    ]

    half = width // HALVES

    def lanes(h):
        return pl.ds(h * half, half)

    def first(u, h):
        c = u // HALVES
        return copy(
            tok_in.at[:, c, :, lanes(h)], raw.at[c, :, :, lanes(h)],
            s0_send.at[u], s0_recv.at[u], to_dp(0),
        )

    def stage(k, u, h, owner):
        size = 1 << k
        base = mirrored(owner, bits) // size * size
        rows = pl.ds(pl.multiple_of(base * ROWS, ROWS), size * ROWS)
        here = tok.at[u // HALVES, rows, lanes(h)]
        return copy(here, here, st_send.at[k - 1, u], st_recv.at[k - 1, u], to_dp(k))

    def near_copy(c, p):
        start = (1 - core) * 2
        return copy(
            part.at[c, :, pl.ds(start, 2), :, span(p)], near.at[c, :, :, :, span(p)],
            nr_send.at[c, p], nr_recv.at[c, p], near_id,
        )

    def far_copy(c, p):
        return copy(
            pair.at[c, :, :, span(p)], far.at[c, :, :, span(p)],
            fr_send.at[c, p], fr_recv.at[c, p], far_id,
        )

    def home_copy(s):
        return copy(
            d_loc.at[s], d_in.at[s, t], ds_send.at[s], ds_recv.at[s, t], {"tensor": homes[s]}
        )

    def home_in(s, other):
        return copy(
            d_in.at[s, other], d_in.at[s, other], ds_send.at[s], ds_recv.at[s, other], near_id
        )

    def spread(s, k):
        return copy(
            d_all.at[s, d], d_all.at[s, d], db_send.at[k], db_recv.at[s, d], {"dp": (d + k) % dp}
        )

    def spread_in(s, source):
        return copy(
            d_all.at[s, source], d_all.at[s, source], db_send.at[0], db_recv.at[s, source],
            {"dp": hops[0]},
        )

    def gm_copy(k):
        return copy(
            gm_in.at[t], gm_in.at[t], gm_send.at[k], gm_recv.at[t], {"tensor": (t + k) % tp}
        )

    def gm_from(k):
        source = (t + k) % tp
        return copy(
            gm_in.at[source], gm_in.at[source], gm_send.at[k], gm_recv.at[source], near_id
        )

    def small(n, src, dst, target):
        return copy(src, dst, ms_send.at[n], ms_recv.at[n], target)

    sq1 = small(0, sq, sq_near, near_id)
    sq2 = small(1, sq_near, sq_far, far_id)
    rp_hops = [small(2 + k, rp.at[k], rp_in.at[k], to_dp(bits - 1 - k)) for k in range(bits)]
    n0 = 2 + bits
    rg1 = small(n0, rgt.at[t], rgt.at[t], near_id)
    rg1_in = small(n0, rgt.at[t_near], rgt.at[t_near], near_id)
    mine2 = pl.ds(side * 2, 2)
    theirs2 = pl.ds((1 - side) * 2, 2)
    rg2 = small(n0 + 1, rgt.at[mine2], rgt.at[mine2], far_id)
    rg2_in = small(n0 + 1, rgt.at[theirs2], rgt.at[theirs2], far_id)
    share = rank // 2
    gb1 = small(n0 + 2, gb_part.at[1 - core], gb_near, near_id)
    gb2 = small(n0 + 3, gb_sum, gb_far, far_id)
    gb3 = small(n0 + 4, gb_all.at[core], gb_all.at[core], near_id)
    gb3_in = small(n0 + 4, gb_all.at[1 - core], gb_all.at[1 - core], near_id)

    def each_tile(body):
        @pl.loop(0, tiles)
        def _(n):
            body(tile_at(n))

    barrier = pltpu.get_barrier_semaphore()

    def greet_dp(k):
        pl.semaphore_signal(barrier, inc=1, device_id={"dp": (d + k) % dp}, device_id_type=MESH)

    @pl.loop(1, dp)
    def _(k):
        greet_dp(k)

    for k in range(1, tp):
        pl.semaphore_signal(barrier, inc=1, device_id={"tensor": (t + k) % tp}, device_id_type=MESH)

    tok_copy.start()
    for load in loads:
        load.start()
    for n in range(tiles):
        w_copy(n).start()
    for load in cot_loads:
        load.start()

    gm_acc[...] = jnp.zeros_like(gm_acc)
    tok_copy.wait()
    pl.semaphore_wait(barrier, dp - 1 + tp - 1)
    for u in range(AHEAD):
        first(u, u % HALVES).start()
    for load in loads:
        load.wait()

    for s in range(2):
        block = tok_in[s].reshape(BLK, width)
        d_loc[s] = dots(down[...], block, 1, 1).astype(BF16)
    for s in range(2):
        when(t != homes[s], lambda: home_copy(s).start())

    gram = dots(down[...], down[...], 1, 1)
    gram_high = gram.astype(BF16)
    gram_low = (gram - gram_high.astype(F32)).astype(BF16)

    own_live = routing[0, d] == d
    pair_live = routing[0, hops[0]] == hops[0]
    depth = 256

    def norm_tile(n):
        w_copy(n).wait()
        at = tile_at(n)
        cross = jnp.dot(down[...], w[:, at], preferred_element_type=F32)
        total = jnp.zeros((16, tile), F32)
        for r in range(0, width, depth):
            block = w[r:r + depth, at].astype(F32)
            total = total + jnp.sum((block * block).reshape(depth // 16, 16, tile), axis=0)
        ups = up[:, at]
        quad = (
            jnp.dot(gram_high, ups, preferred_element_type=F32)
            + jnp.dot(gram_low, ups, preferred_element_type=F32)
        )
        mixed = (2.0 * scale * cross + scale * scale * quad) * ups.astype(F32)
        sq[:, at] = (
            jnp.sum(total, axis=0, keepdims=True) + jnp.sum(mixed, axis=0, keepdims=True)
        )

    def gradient():
        def body(at):
            square = sq_near[:, at] + sq_far[:, at]
            size = jnp.sqrt(jnp.maximum(square, 0.25))
            ratio = mag[at].reshape(1, tile) / size
            norm[:, at] = size
            factor[:, at] = ratio
            for g in range(per):
                sg[g, :, at] = (cot[g, :, at].astype(F32) * ratio * inverse).astype(BF16)

        each_tile(body)
        for g in range(per):
            rp[0, :, g * BLK:(g + 1) * BLK] = dots(up[...], sg[g], 1, 1)

    def gather_down():
        for s in range(2):
            @pl.when(t == homes[s])
            def _():
                d_in[s, t] = d_loc[s]
                for k in range(1, tp):
                    home_in(s, (t + k) % tp).wait_recv()
                total = d_in[s, 0].astype(F32)
                for other in range(1, tp):
                    total = total + d_in[s, other].astype(F32)
                d_all[s, d] = total.astype(BF16)

                @pl.loop(1, dp)
                def _(k):
                    spread(s, k).start()

    def take_down():
        for g in range(per):
            p = t * per + g
            across = flipped(p, dp // 2)
            when(p != d, lambda: spread_in(0, p).wait_recv())
            when(across != d, lambda: spread_in(1, across).wait_recv())
            live = routing[0, p] == p
            turned = jnp.where(live, d_all[0, p], d_all[1, across])
            proj_turned[:, order[g] * BLK:(order[g] + 1) * BLK] = turned
            proj_down[order[g]] = turned.astype(F32).T.astype(BF16)

    def multiply(c, p):
        for n in range(*pieces[p]):
            at = tile_at(n)
            prod = jnp.dot(tok[c], w[:, at], preferred_element_type=F32)
            part[c, :, :, :, at] = prod.astype(BF16).reshape(per, tp, ROWS, tile)
        near_copy(c, p).start()

    def combine(c, p):
        near_copy(c, p).wait_recv()
        other = core * 2 + 1 - side
        for n in range(*pieces[p]):
            at = tile_at(n)
            pair[c, :, :, at] = (
                part[c, :, other, :, at].astype(F32) + near[c, :, 1 - side, :, at].astype(F32)
            ).astype(BF16)
        far_copy(c, p).start()

    def epilogue(c, p):
        far_copy(c, p).wait_recv()
        mine = core * 2 + side
        rows = pl.ds(pl.multiple_of(c * ROWS, ROWS), ROWS)
        lhs = proj_down[:, rows, :].reshape(high, rank)
        for n in range(*pieces[p]):
            at = tile_at(n)
            total = (
                part[c, :, mine, :, at].astype(F32)
                + near[c, :, side, :, at].astype(F32)
                + far[c, :, :, at].astype(F32)
            ).reshape(high, tile)
            pre = total + scale * jnp.dot(lhs, up[:, at], preferred_element_type=F32)
            out[:, rows, at] = (pre * factor[:, at]).astype(BF16).reshape(per, ROWS, tile)
            both = cot[:, rows, at].astype(F32).reshape(high, tile) * pre
            gm_acc[:, at] += jnp.sum(both.reshape(high // 8, 8, tile), axis=0)

    def gb_start():
        for n in range(tiles):
            at = tile_at(n)
            gb_part[:, :, at] = (
                scale * jnp.dot(
                    proj_turned[...], sg[:, :, at].reshape(per * BLK, tile),
                    preferred_element_type=F32,
                )
            ).astype(BF16).reshape(2, share, tile)
        gb1.start()

    def turn_rows():
        for s in range(tp):
            turned = rgt[s].astype(F32).T.astype(BF16)
            spot = s % 2 * 2 + s // 2
            for g in range(per):
                rg[:, g, spot] = turned[g * BLK:(g + 1) * BLK].reshape(CHUNKS, ROWS, rank)
        rg_turned[...] = rg[...].reshape(dp * BLK, rank).astype(F32).T.astype(BF16)

    for n in range(min(EARLY, tiles)):
        norm_tile(n)

    later = max(0, tiles - EARLY)
    norm_last = -(-later // 2)
    grad_at = norm_last + 2
    gap = max(1, (UNITS - grad_at) // (bits + 1))
    ready = LAG * (bits - 1) + 1
    steps = UNITS + ready + 1
    steps = steps + steps % 2
    gb_at = ready + 3

    @pl.loop(0, steps // 2)
    def _(pass_):
        for h in range(2):
            u = pass_ * 2 + h

            @pl.when(u < UNITS)
            def _():
                first(u, h).wait_recv()
                c = u // HALVES
                at = lanes(h)
                own_at = pl.ds(pl.multiple_of(mirrored(d, bits) * ROWS, ROWS), ROWS)
                pair_at = pl.ds(pl.multiple_of(mirrored(hops[0], bits) * ROWS, ROWS), ROWS)
                tok[c, own_at, at] = jnp.where(own_live, tok_in[0, c, :, at], raw[c, 1, :, at])
                tok[c, pair_at, at] = jnp.where(pair_live, raw[c, 0, :, at], tok_in[1, c, :, at])
                stage(1, u, h, d).start()

            when(u + AHEAD < UNITS, lambda: first(u + AHEAD, (h + AHEAD) % 2).start())

            for k in range(1, bits):
                v = u - LAG * k
                hv = (h - LAG * k) % 2

                @pl.when((v >= 0) & (v < UNITS))
                def _():
                    stage(k, v, hv, hops[k]).wait_recv()
                    if k < bits - 1:
                        stage(k + 1, v, hv, d).start()

            @pl.when((u >= 1) & (u <= norm_last))
            def _():
                for e in range(2):
                    n = EARLY + (u - 1) * 2 + e
                    when(n < tiles, lambda: norm_tile(n))

            when(u == 1, gather_down)
            when(u == norm_last, lambda: sq1.start())

            @pl.when(u == norm_last + 1)
            def _():
                sq1.wait()
                sq_near[...] = sq_near[...] + sq[...]
                sq2.start()

            @pl.when(u == grad_at)
            def _():
                sq2.wait()
                for load in cot_loads:
                    load.wait()
                gradient()
                rp_hops[0].start()

            when(u == ready, take_down)

            for k in range(bits):
                @pl.when(u == grad_at + gap * (k + 1))
                def _():
                    rp_hops[k].wait()
                    merged = rp[k] + rp_in[k]
                    if k < bits - 1:
                        rp[k + 1] = merged
                        rp_hops[k + 1].start()
                    else:
                        rgt[t] = merged.astype(BF16)
                        rg1.start()

            @pl.when(u == grad_at + gap * bits + 1)
            def _():
                rg1.wait_send()
                rg1_in.wait_recv()
                rg2.start()

            @pl.when(u == grad_at + gap * bits + 3)
            def _():
                rg2.wait_send()
                rg2_in.wait_recv()
                turn_rows()

            m = u - ready
            hm = (h - ready) % 2
            when((m >= 0) & (m < UNITS), lambda: multiply(m // 2, hm))
            when((m >= 1) & (m <= UNITS), lambda: combine((m - 1) // 2, 1 - hm))
            when((m >= 3) & (m <= UNITS), lambda: epilogue((m - 3) // 2, 1 - hm))

            when(u == gb_at, gb_start)

            @pl.when(u == gb_at + 2)
            def _():
                gb1.wait()
                gb_sum[...] = (gb_part[core].astype(F32) + gb_near[...].astype(F32)).astype(BF16)
                gb2.start()

            @pl.when(u == gb_at + 6)
            def _():
                gb2.wait()
                gb_all[core] = gb_sum[...].astype(F32) + gb_far[...].astype(F32)
                gb3.start()

            @pl.when(u == gb_at + 8)
            def _():
                gb3.wait_send()
                gb3_in.wait_recv()
                gb_out[...] = gb_all[...].reshape(rank, cols)

    wide = min(512, width)

    @pl.loop(0, width // wide)
    def _(n):
        at = pl.ds(pl.multiple_of(n * wide, wide), wide)
        ga_out[:, at] = scale * jnp.dot(
            rg_turned[...], tok[:, :, at].reshape(dp * BLK, wide), preferred_element_type=F32
        )

    @pl.loop(0, CHUNKS)
    def _(c):
        for h in range(HALVES):
            u = c * HALVES + h
            first(u, h).wait_send()
            for k in range(1, bits):
                stage(k, u, h, d).wait_send()
        for p in range(2):
            near_copy(c, p).wait_send()

    for s in range(2):
        when(t != homes[s], lambda: home_copy(s).wait_send())

        @pl.when(t == homes[s])
        def _():
            @pl.loop(1, dp)
            def _(k):
                spread(s, k).wait_send()

    for q in range(UNITS - 2, UNITS):
        epilogue(q // 2, q % 2)

    gm_in[t] = jnp.sum(gm_acc[...], axis=0, keepdims=True) / norm[...] * inverse
    for k in range(1, tp):
        gm_copy(k).start()

    @pl.loop(0, CHUNKS)
    def _(c):
        for p in range(2):
            far_copy(c, p).wait_send()

    for k in range(1, tp):
        gm_from(k).wait_recv()
    total = gm_in[0]
    for s in range(1, tp):
        total = total + gm_in[s]
    gm_out[...] = total.reshape(cols)
    for k in range(1, tp):
        gm_copy(k).wait_send()


def finish(order, out, ga, gb, gm, out_hbm, ga_hbm, gb_hbm, gm_hbm, sem):
    moves = [
        pltpu.make_async_copy(out.at[order[g]], out_hbm.at[g], sem.at[g])
        for g in range(len(order))
    ]
    for src, dst in ((ga, ga_hbm), (gb, gb_hbm), (gm, gm_hbm)):
        moves.append(pltpu.make_async_copy(src, dst, sem.at[len(moves)]))
    for move in moves:
        move.start()
    for move in moves:
        move.wait()


def body(dp, tp, tokens, routing, weight, down, up, mag, cot):
    width, cols = weight.shape
    rank = down.shape[0]
    per = dp // tp
    bits = dp.bit_length() - 1
    tile = next(size for size in (512, 256, 128) if cols % size == 0)
    tiles = cols // tile
    cfg = (dp, tp, width, cols, rank, tile)
    vmem = pl.BlockSpec(memory_space=pltpu.VMEM)
    hbm = pl.BlockSpec(memory_space=pltpu.HBM)
    dma = pltpu.SemaphoreType.DMA
    mine = per * BLK
    shapes = (
        ((per, BLK, cols), BF16),
        ((rank, width), F32),
        ((rank, cols), F32),
        ((cols,), F32),
    )
    held = pl.pallas_call(
        functools.partial(kernel, cfg),
        out_shape=tuple(OUT(shape, kind) for shape, kind in shapes),
        in_specs=[hbm, pl.BlockSpec(memory_space=pltpu.SMEM), hbm, hbm, hbm, hbm, hbm],
        out_specs=(vmem, vmem, vmem, vmem),
        scratch_shapes=[
            pltpu.VMEM((2, CHUNKS, ROWS, width), BF16),
            pltpu.VMEM((rank, width), BF16),
            pltpu.VMEM((rank, cols), BF16),
            pltpu.VMEM((cols,), F32),
            pltpu.VMEM((per, BLK, cols), BF16),
            pltpu.VMEM((width, cols), BF16),
            pltpu.VMEM((CHUNKS, 2, ROWS, width), BF16),
            pltpu.VMEM((CHUNKS, dp * ROWS, width), BF16),
            pltpu.VMEM((CHUNKS, per, tp, ROWS, cols), BF16),
            pltpu.VMEM((CHUNKS, per, 2, ROWS, cols), BF16),
            pltpu.VMEM((CHUNKS, per, ROWS, cols), BF16),
            pltpu.VMEM((CHUNKS, per, ROWS, cols), BF16),
            pltpu.VMEM((1, cols), F32),
            pltpu.VMEM((1, cols), F32),
            pltpu.VMEM((1, cols), F32),
            pltpu.VMEM((1, cols), F32),
            pltpu.VMEM((1, cols), F32),
            pltpu.VMEM((per, BLK, cols), BF16),
            pltpu.VMEM((bits, rank, mine), F32),
            pltpu.VMEM((bits, rank, mine), F32),
            pltpu.VMEM((tp, rank, mine), BF16),
            pltpu.VMEM((CHUNKS, per, tp, ROWS, rank), BF16),
            pltpu.VMEM((rank, dp * BLK), BF16),
            pltpu.VMEM((per, BLK, rank), BF16),
            pltpu.VMEM((rank, mine), BF16),
            pltpu.VMEM((8, cols), F32),
            pltpu.VMEM((2, rank // 2, cols), BF16),
            pltpu.VMEM((rank // 2, cols), BF16),
            pltpu.VMEM((rank // 2, cols), BF16),
            pltpu.VMEM((rank // 2, cols), BF16),
            pltpu.VMEM((2, rank // 2, cols), F32),
            pltpu.VMEM((tp, 1, cols), F32),
            pltpu.VMEM((2, rank, BLK), BF16),
            pltpu.VMEM((2, tp, rank, BLK), BF16),
            pltpu.VMEM((2, dp, rank, BLK), BF16),
            dma((4 + per,)),
            dma((tiles,)),
            dma((UNITS,)), dma((UNITS,)),
            dma((bits - 1, UNITS)), dma((bits - 1, UNITS)),
            dma((CHUNKS, 2)), dma((CHUNKS, 2)),
            dma((CHUNKS, 2)), dma((CHUNKS, 2)),
            dma((bits + 7,)), dma((bits + 7,)),
            dma((2,)), dma((2, tp)),
            dma((dp,)), dma((2, dp)),
            dma((tp,)), dma((tp,)),
        ],
        compiler_params=pltpu.CompilerParams(
            collective_id=0, has_side_effects=True, vmem_limit_bytes=LIMIT
        ),
    )(
        tokens.reshape(2, CHUNKS, ROWS, width),
        routing.T,
        weight,
        down,
        up,
        mag,
        cot.reshape(per, BLK, cols),
    )
    order = [mirrored(g, per.bit_length() - 1) for g in range(per)]
    out, ga, gb, gm = pl.pallas_call(
        functools.partial(finish, order),
        out_shape=tuple(jax.ShapeDtypeStruct(shape, kind) for shape, kind in shapes),
        in_specs=[vmem, vmem, vmem, vmem],
        out_specs=(hbm, hbm, hbm, hbm),
        scratch_shapes=[dma((per + 3,))],
    )(*(pltpu.with_memory_space_constraint(x, pltpu.VMEM) for x in held))
    return out.reshape(mine, cols), ga, gb, gm


OUT = pltpu.VMEM
LIMIT = 56 * 1024 * 1024


def solution(mesh):
    return jax.shard_map(
        functools.partial(body, mesh.shape["dp"], mesh.shape["tensor"]),
        mesh=mesh,
        in_specs=(
            P("dp", "tensor"),
            P(),
            P("tensor", "dp"),
            P(None, "tensor"),
            P(None, "dp"),
            P("dp"),
            P("tensor", "dp"),
        ),
        out_specs=(P("tensor", "dp"), P(None, "tensor"), P(None, "dp"), P("dp")),
        check_vma=False,
    )
```

```python
import functools
import math

import jax
import jax.numpy as jnp
from jax import lax
from jax.experimental import pallas as pl
from jax.experimental.pallas import tpu as pltpu
from jax.sharding import PartitionSpec as P

BLK = 128
ROWS = 16
CHUNKS = BLK // ROWS
HALVES = 4
UNITS = CHUNKS * HALVES
AHEAD = 4
LAG = 3
EARLY = 3
PAIR_LAG = 1
END_LAG = 4
RING = HALVES * -(-(2 * max(AHEAD, LAG, PAIR_LAG, END_LAG) + 2) // HALVES)
MESH = pl.DeviceIdType.MESH
F32 = jnp.float32
BF16 = jnp.bfloat16


def mirrored(value, bits):
    result = 0
    for position in range(bits):
        result = result + (value // (1 << position)) % 2 * (1 << (bits - 1 - position))
    return result


def flipped(value, bit):
    return value + bit - 2 * bit * ((value // bit) % 2)


def dots(left, right, left_dim, right_dim):
    return lax.dot_general(
        left, right, (((left_dim,), (right_dim,)), ((), ())), preferred_element_type=F32
    )


def kernel(
    cfg,
    tok_hbm, routing, w_hbm, down_hbm, up_hbm, mag_hbm, cot_hbm,
    out, ga_out, gb_out, gm_out,
    tok_in, down, up, mag, cot, w,
    raw, tok, part, near, pair, far, sq, sq_near, sq_far, factor, norm, sg,
    rp, rp_in, rgt, rg, rg_turned, proj_down, proj_turned, gm_acc,
    gb_part, gb_near, gb_sum, gb_far, gb_all, gm_in, d_loc, d_in, d_all,
    in_sem, w_sem, s0_send, s0_recv, st_send, st_recv, nr_send, nr_recv, fr_send, fr_recv,
    ms_send, ms_recv, ds_send, ds_recv, db_send, db_recv, gm_send, gm_recv,
):
    dp, tp, width, cols, rank, tile = cfg
    bits = dp.bit_length() - 1
    per = dp // tp
    tiles = cols // tile
    cut = -(-tiles // HALVES)
    pieces = [(min(p * cut, tiles), min((p + 1) * cut, tiles)) for p in range(HALVES)]
    order = [mirrored(g, per.bit_length() - 1) for g in range(per)]
    scale = 1.0 / math.sqrt(rank)
    inverse = 1.0 / math.sqrt(dp * BLK)
    high = per * ROWS
    d = lax.axis_index("dp")
    t = lax.axis_index("tensor")
    core = t % 2
    side = t // 2
    t_near, t_far = flipped(t, 1), flipped(t, 2)
    hops = [flipped(d, dp >> (k + 1)) for k in range(bits)]
    homes = (d // per, hops[0] // per)

    def copy(src, dst, send, recv, target):
        return pltpu.make_async_remote_copy(
            src_ref=src, dst_ref=dst, send_sem=send, recv_sem=recv,
            device_id=target, device_id_type=MESH,
        )

    def when(condition, action):
        pl.when(condition)(action)

    def send(make, u, *rest):
        when(u >= RING, lambda: make(u - RING, *rest).wait_send())
        make(u, *rest).start()

    def send_piece(make, c, p):
        back = RING // HALVES
        when(c >= back, lambda: make(c - back, p).wait_send())
        make(c, p).start()

    def to_dp(k):
        return {"dp": hops[k]}

    near_id, far_id = {"tensor": t_near}, {"tensor": t_far}

    def span(p):
        return pl.ds(pieces[p][0] * tile, (pieces[p][1] - pieces[p][0]) * tile)

    def tile_at(n):
        if isinstance(n, int):
            return pl.ds(n * tile, tile)
        return pl.ds(pl.multiple_of(n * tile, tile), tile)

    def w_copy(n):
        return pltpu.make_async_copy(w_hbm.at[:, tile_at(n)], w.at[:, tile_at(n)], w_sem.at[n])

    lead = pl.ds(0, 2)
    rest = pl.ds(2, CHUNKS - 2)
    tok_lead = pltpu.make_async_copy(tok_hbm.at[:, lead], tok_in.at[:, lead], in_sem.at[0])
    tok_rest = pltpu.make_async_copy(tok_hbm.at[:, rest], tok_in.at[:, rest], in_sem.at[4 + per])
    loads = [
        pltpu.make_async_copy(down_hbm, down, in_sem.at[1]),
        pltpu.make_async_copy(up_hbm, up, in_sem.at[2]),
        pltpu.make_async_copy(mag_hbm, mag, in_sem.at[3]),
    ]
    cot_loads = [
        pltpu.make_async_copy(cot_hbm.at[g], cot.at[order[g]], in_sem.at[4 + g])
        for g in range(per)
    ]

    half = width // HALVES

    def lanes(h):
        return pl.ds(h * half, half)

    def first(u, h):
        c = u // HALVES
        return copy(
            tok_in.at[:, c, :, lanes(h)], raw.at[c, :, :, lanes(h)],
            s0_send.at[u % RING], s0_recv.at[u % RING], to_dp(0),
        )

    def stage(k, u, h, owner):
        size = 1 << k
        base = mirrored(owner, bits) // size * size
        rows = pl.ds(pl.multiple_of(base * ROWS, ROWS), size * ROWS)
        here = tok.at[u // HALVES, rows, lanes(h)]
        n = u % RING
        return copy(here, here, st_send.at[k - 1, n], st_recv.at[k - 1, n], to_dp(k))

    def near_copy(c, p):
        n = (c * HALVES + p) % RING
        start = (1 - core) * 2
        return copy(
            part.at[c, :, pl.ds(start, 2), :, span(p)], near.at[c, :, :, :, span(p)],
            nr_send.at[n], nr_recv.at[n], near_id,
        )

    def far_copy(c, p):
        n = (c * HALVES + p) % RING
        return copy(
            pair.at[c, :, :, span(p)], far.at[c, :, :, span(p)],
            fr_send.at[n], fr_recv.at[n], far_id,
        )

    def home_copy(s):
        return copy(
            d_loc.at[s], d_in.at[s, t], ds_send.at[s], ds_recv.at[s, t], {"tensor": homes[s]}
        )

    def home_in(s, other):
        return copy(
            d_in.at[s, other], d_in.at[s, other], ds_send.at[s], ds_recv.at[s, other], near_id
        )

    def spread(s, k):
        return copy(
            d_all.at[s, d], d_all.at[s, d], db_send.at[k], db_recv.at[s, d], {"dp": (d + k) % dp}
        )

    def spread_in(s, source):
        return copy(
            d_all.at[s, source], d_all.at[s, source], db_send.at[0], db_recv.at[s, source],
            {"dp": hops[0]},
        )

    def gm_copy(k):
        return copy(
            gm_in.at[t], gm_in.at[t], gm_send.at[k], gm_recv.at[t], {"tensor": (t + k) % tp}
        )

    def gm_from(k):
        source = (t + k) % tp
        return copy(
            gm_in.at[source], gm_in.at[source], gm_send.at[k], gm_recv.at[source], near_id
        )

    def small(n, src, dst, target):
        return copy(src, dst, ms_send.at[n], ms_recv.at[n], target)

    sq1 = small(0, sq, sq_near, near_id)
    sq2 = small(1, sq_near, sq_far, far_id)
    rp_hops = [small(2 + k, rp.at[k], rp_in.at[k], to_dp(bits - 1 - k)) for k in range(bits)]
    n0 = 2 + bits
    rg1 = small(n0, rgt.at[t], rgt.at[t], near_id)
    rg1_in = small(n0, rgt.at[t_near], rgt.at[t_near], near_id)
    mine2 = pl.ds(side * 2, 2)
    theirs2 = pl.ds((1 - side) * 2, 2)
    rg2 = small(n0 + 1, rgt.at[mine2], rgt.at[mine2], far_id)
    rg2_in = small(n0 + 1, rgt.at[theirs2], rgt.at[theirs2], far_id)
    share = rank // 2
    gb1 = small(n0 + 2, gb_part.at[1 - core], gb_near, near_id)
    gb2 = small(n0 + 3, gb_sum, gb_far, far_id)
    gb3 = small(n0 + 4, gb_all.at[core], gb_all.at[core], near_id)
    gb3_in = small(n0 + 4, gb_all.at[1 - core], gb_all.at[1 - core], near_id)

    def each_tile(body):
        @pl.loop(0, tiles)
        def _(n):
            body(tile_at(n))

    tok_lead.start()
    barrier = pltpu.get_barrier_semaphore()

    def greet_dp(k):
        pl.semaphore_signal(barrier, inc=1, device_id={"dp": (d + k) % dp}, device_id_type=MESH)

    @pl.loop(1, dp)
    def _(k):
        greet_dp(k)

    for k in range(1, tp):
        pl.semaphore_signal(barrier, inc=1, device_id={"tensor": (t + k) % tp}, device_id_type=MESH)

    tok_rest.start()
    for load in loads:
        load.start()
    for n in range(tiles):
        w_copy(n).start()
    for load in cot_loads:
        load.start()

    gm_acc[...] = jnp.zeros_like(gm_acc)
    tok_lead.wait()
    pl.semaphore_wait(barrier, dp - 1 + tp - 1)
    for u in range(AHEAD):
        first(u, u % HALVES).start()
    tok_rest.wait()
    for load in loads:
        load.wait()

    for s in range(2):
        block = tok_in[s].reshape(BLK, width)
        d_loc[s] = dots(down[...], block, 1, 1).astype(BF16)
    for s in range(2):
        when(t != homes[s], lambda: home_copy(s).start())

    gram = dots(down[...], down[...], 1, 1)
    gram_high = gram.astype(BF16)
    gram_low = (gram - gram_high.astype(F32)).astype(BF16)

    own_live = routing[0, d] == d
    pair_live = routing[0, hops[0]] == hops[0]
    depth = 256

    def norm_tile(n):
        w_copy(n).wait()
        at = tile_at(n)
        cross = jnp.dot(down[...], w[:, at], preferred_element_type=F32)
        total = jnp.zeros((16, tile), F32)
        for r in range(0, width, depth):
            block = w[r:r + depth, at].astype(F32)
            total = total + jnp.sum((block * block).reshape(depth // 16, 16, tile), axis=0)
        ups = up[:, at]
        quad = (
            jnp.dot(gram_high, ups, preferred_element_type=F32)
            + jnp.dot(gram_low, ups, preferred_element_type=F32)
        )
        mixed = (2.0 * scale * cross + scale * scale * quad) * ups.astype(F32)
        sq[:, at] = (
            jnp.sum(total, axis=0, keepdims=True) + jnp.sum(mixed, axis=0, keepdims=True)
        )

    def gradient():
        def body(at):
            square = sq_near[:, at] + sq_far[:, at]
            size = jnp.sqrt(jnp.maximum(square, 0.25))
            ratio = mag[at].reshape(1, tile) / size
            norm[:, at] = size
            factor[:, at] = ratio
            for g in range(per):
                sg[g, :, at] = (cot[g, :, at].astype(F32) * ratio * inverse).astype(BF16)

        each_tile(body)
        for g in range(per):
            rp[0, :, g * BLK:(g + 1) * BLK] = dots(up[...], sg[g], 1, 1)

    def gather_down():
        for s in range(2):
            @pl.when(t == homes[s])
            def _():
                d_in[s, t] = d_loc[s]
                for k in range(1, tp):
                    home_in(s, (t + k) % tp).wait_recv()
                total = d_in[s, 0].astype(F32)
                for other in range(1, tp):
                    total = total + d_in[s, other].astype(F32)
                d_all[s, d] = total.astype(BF16)

                @pl.loop(1, dp)
                def _(k):
                    spread(s, k).start()

    def take_down():
        for g in range(per):
            p = t * per + g
            across = flipped(p, dp // 2)
            when(p != d, lambda: spread_in(0, p).wait_recv())
            when(across != d, lambda: spread_in(1, across).wait_recv())
            live = routing[0, p] == p
            turned = jnp.where(live, d_all[0, p], d_all[1, across])
            proj_turned[:, order[g] * BLK:(order[g] + 1) * BLK] = turned
            proj_down[order[g]] = turned.astype(F32).T.astype(BF16)

    def multiply(c, p):
        for n in range(*pieces[p]):
            at = tile_at(n)
            prod = jnp.dot(tok[c], w[:, at], preferred_element_type=F32)
            part[c, :, :, :, at] = prod.astype(BF16).reshape(per, tp, ROWS, tile)
        send_piece(near_copy, c, p)

    def combine(c, p):
        near_copy(c, p).wait_recv()
        other = core * 2 + 1 - side
        for n in range(*pieces[p]):
            at = tile_at(n)
            pair[c, :, :, at] = (
                part[c, :, other, :, at].astype(F32) + near[c, :, 1 - side, :, at].astype(F32)
            ).astype(BF16)
        send_piece(far_copy, c, p)

    def epilogue(c, p):
        far_copy(c, p).wait_recv()
        mine = core * 2 + side
        rows = pl.ds(pl.multiple_of(c * ROWS, ROWS), ROWS)
        lhs = proj_down[:, rows, :].reshape(high, rank)
        for n in range(*pieces[p]):
            at = tile_at(n)
            total = (
                part[c, :, mine, :, at].astype(F32)
                + near[c, :, side, :, at].astype(F32)
                + far[c, :, :, at].astype(F32)
            ).reshape(high, tile)
            pre = total + scale * jnp.dot(lhs, up[:, at], preferred_element_type=F32)
            out[:, rows, at] = (pre * factor[:, at]).astype(BF16).reshape(per, ROWS, tile)
            both = cot[:, rows, at].astype(F32).reshape(high, tile) * pre
            gm_acc[:, at] += jnp.sum(both.reshape(high // 8, 8, tile), axis=0)

    def gb_start():
        for n in range(tiles):
            at = tile_at(n)
            gb_part[:, :, at] = (
                scale * jnp.dot(
                    proj_turned[...], sg[:, :, at].reshape(per * BLK, tile),
                    preferred_element_type=F32,
                )
            ).astype(BF16).reshape(2, share, tile)
        gb1.start()

    def turn_rows():
        for s in range(tp):
            turned = rgt[s].astype(F32).T.astype(BF16)
            spot = s % 2 * 2 + s // 2
            for g in range(per):
                rg[:, g, spot] = turned[g * BLK:(g + 1) * BLK].reshape(CHUNKS, ROWS, rank)
        rg_turned[...] = rg[...].reshape(dp * BLK, rank).astype(F32).T.astype(BF16)

    for n in range(min(EARLY, tiles)):
        norm_tile(n)

    later = max(0, tiles - EARLY)
    norm_last = max(1, later)
    grad_at = norm_last + 8
    gap = max(1, (UNITS - grad_at) // (bits + 1))
    ready = LAG * (bits - 1) + HALVES - 1
    steps = -(-(UNITS + ready + PAIR_LAG) // HALVES) * HALVES
    gb_at = grad_at + 4

    @pl.loop(0, steps // HALVES)
    def _(pass_):
        for h in range(HALVES):
            u = pass_ * HALVES + h

            @pl.when(u < UNITS)
            def _():
                first(u, h).wait_recv()
                c = u // HALVES
                at = lanes(h)
                own_at = pl.ds(pl.multiple_of(mirrored(d, bits) * ROWS, ROWS), ROWS)
                pair_at = pl.ds(pl.multiple_of(mirrored(hops[0], bits) * ROWS, ROWS), ROWS)
                tok[c, own_at, at] = jnp.where(own_live, tok_in[0, c, :, at], raw[c, 1, :, at])
                tok[c, pair_at, at] = jnp.where(pair_live, raw[c, 0, :, at], tok_in[1, c, :, at])
                send(functools.partial(stage, 1), u, h, d)

            when(u + AHEAD < UNITS, lambda: send(first, u + AHEAD, (h + AHEAD) % HALVES))

            for k in range(1, bits):
                v = u - LAG * k
                hv = (h - LAG * k) % HALVES

                @pl.when((v >= 0) & (v < UNITS))
                def _():
                    stage(k, v, hv, hops[k]).wait_recv()
                    if k < bits - 1:
                        send(functools.partial(stage, k + 1), v, hv, d)

            @pl.when((u >= 1) & (u <= norm_last))
            def _():
                n = EARLY + u - 1
                when(n < tiles, lambda: norm_tile(n))

            when(u == 2, gather_down)
            when(u == norm_last, lambda: sq1.start())

            @pl.when(u == norm_last + 4)
            def _():
                sq1.wait()
                sq_near[...] = sq_near[...] + sq[...]
                sq2.start()

            @pl.when(u == grad_at)
            def _():
                sq2.wait()
                for load in cot_loads:
                    load.wait()
                gradient()
                rp_hops[0].start()

            when(u == grad_at + 2, take_down)

            for k in range(bits):
                @pl.when(u == grad_at + gap * (k + 1))
                def _():
                    rp_hops[k].wait()
                    merged = rp[k] + rp_in[k]
                    if k < bits - 1:
                        rp[k + 1] = merged
                        rp_hops[k + 1].start()
                    else:
                        rgt[t] = merged.astype(BF16)
                        rg1.start()

            @pl.when(u == grad_at + gap * bits + 2)
            def _():
                rg1.wait_send()
                rg1_in.wait_recv()
                rg2.start()

            @pl.when(u == grad_at + gap * bits + 6)
            def _():
                rg2.wait_send()
                rg2_in.wait_recv()
                turn_rows()

            m = u - ready
            mq = m - PAIR_LAG
            me = mq - END_LAG
            at_m, at_q, at_e = (
                (h - ready - lag) % HALVES for lag in (0, PAIR_LAG, PAIR_LAG + END_LAG)
            )
            when((m >= 0) & (m < UNITS), lambda: multiply(m // HALVES, at_m))
            when((mq >= 0) & (mq < UNITS), lambda: combine(mq // HALVES, at_q))
            when((me >= 0) & (me < UNITS - END_LAG), lambda: epilogue(me // HALVES, at_e))

            when(u == gb_at, gb_start)

            @pl.when(u == gb_at + 3)
            def _():
                gb1.wait()
                gb_sum[...] = (gb_part[core].astype(F32) + gb_near[...].astype(F32)).astype(BF16)
                gb2.start()

            @pl.when(u == gb_at + 9)
            def _():
                gb2.wait()
                gb_all[core] = gb_sum[...].astype(F32) + gb_far[...].astype(F32)
                gb3.start()

            @pl.when(u == gb_at + 12)
            def _():
                gb3.wait_send()
                gb3_in.wait_recv()
                gb_out[...] = gb_all[...].reshape(rank, cols)

    wide = min(512, width)

    @pl.loop(0, width // wide)
    def _(n):
        at = pl.ds(pl.multiple_of(n * wide, wide), wide)
        ga_out[:, at] = scale * jnp.dot(
            rg_turned[...], tok[:, :, at].reshape(dp * BLK, wide), preferred_element_type=F32
        )

    @pl.loop(CHUNKS - RING // HALVES, CHUNKS)
    def _(c):
        for h in range(HALVES):
            u = c * HALVES + h
            first(u, h).wait_send()
            for k in range(1, bits):
                stage(k, u, h, d).wait_send()
        for p in range(HALVES):
            near_copy(c, p).wait_send()

    for s in range(2):
        when(t != homes[s], lambda: home_copy(s).wait_send())

        @pl.when(t == homes[s])
        def _():
            @pl.loop(1, dp)
            def _(k):
                spread(s, k).wait_send()

    for q in range(UNITS - END_LAG, UNITS):
        epilogue(q // HALVES, q % HALVES)

    gm_in[t] = jnp.sum(gm_acc[...], axis=0, keepdims=True) / norm[...] * inverse
    for k in range(1, tp):
        gm_copy(k).start()

    @pl.loop(CHUNKS - RING // HALVES, CHUNKS)
    def _(c):
        for p in range(HALVES):
            far_copy(c, p).wait_send()

    for k in range(1, tp):
        gm_from(k).wait_recv()
    total = gm_in[0]
    for s in range(1, tp):
        total = total + gm_in[s]
    gm_out[...] = total.reshape(cols)
    for k in range(1, tp):
        gm_copy(k).wait_send()


def finish(order, out, ga, gb, gm, out_hbm, ga_hbm, gb_hbm, gm_hbm, sem):
    moves = [
        pltpu.make_async_copy(out.at[order[g]], out_hbm.at[g], sem.at[g])
        for g in range(len(order))
    ]
    for src, dst in ((ga, ga_hbm), (gb, gb_hbm), (gm, gm_hbm)):
        moves.append(pltpu.make_async_copy(src, dst, sem.at[len(moves)]))
    for move in moves:
        move.start()
    for move in moves:
        move.wait()


def body(dp, tp, tokens, routing, weight, down, up, mag, cot):
    width, cols = weight.shape
    rank = down.shape[0]
    per = dp // tp
    bits = dp.bit_length() - 1
    tile = next(size for size in (512, 256, 128) if cols % size == 0)
    tiles = cols // tile
    cfg = (dp, tp, width, cols, rank, tile)
    vmem = pl.BlockSpec(memory_space=pltpu.VMEM)
    hbm = pl.BlockSpec(memory_space=pltpu.HBM)
    dma = pltpu.SemaphoreType.DMA
    mine = per * BLK
    shapes = (
        ((per, BLK, cols), BF16),
        ((rank, width), F32),
        ((rank, cols), F32),
        ((cols,), F32),
    )
    held = pl.pallas_call(
        functools.partial(kernel, cfg),
        out_shape=tuple(OUT(shape, kind) for shape, kind in shapes),
        in_specs=[hbm, pl.BlockSpec(memory_space=pltpu.SMEM), hbm, hbm, hbm, hbm, hbm],
        out_specs=(vmem, vmem, vmem, vmem),
        scratch_shapes=[
            pltpu.VMEM((2, CHUNKS, ROWS, width), BF16),
            pltpu.VMEM((rank, width), BF16),
            pltpu.VMEM((rank, cols), BF16),
            pltpu.VMEM((cols,), F32),
            pltpu.VMEM((per, BLK, cols), BF16),
            pltpu.VMEM((width, cols), BF16),
            pltpu.VMEM((CHUNKS, 2, ROWS, width), BF16),
            pltpu.VMEM((CHUNKS, dp * ROWS, width), BF16),
            pltpu.VMEM((CHUNKS, per, tp, ROWS, cols), BF16),
            pltpu.VMEM((CHUNKS, per, 2, ROWS, cols), BF16),
            pltpu.VMEM((CHUNKS, per, ROWS, cols), BF16),
            pltpu.VMEM((CHUNKS, per, ROWS, cols), BF16),
            pltpu.VMEM((1, cols), F32),
            pltpu.VMEM((1, cols), F32),
            pltpu.VMEM((1, cols), F32),
            pltpu.VMEM((1, cols), F32),
            pltpu.VMEM((1, cols), F32),
            pltpu.VMEM((per, BLK, cols), BF16),
            pltpu.VMEM((bits, rank, mine), F32),
            pltpu.VMEM((bits, rank, mine), F32),
            pltpu.VMEM((tp, rank, mine), BF16),
            pltpu.VMEM((CHUNKS, per, tp, ROWS, rank), BF16),
            pltpu.VMEM((rank, dp * BLK), BF16),
            pltpu.VMEM((per, BLK, rank), BF16),
            pltpu.VMEM((rank, mine), BF16),
            pltpu.VMEM((8, cols), F32),
            pltpu.VMEM((2, rank // 2, cols), BF16),
            pltpu.VMEM((rank // 2, cols), BF16),
            pltpu.VMEM((rank // 2, cols), BF16),
            pltpu.VMEM((rank // 2, cols), BF16),
            pltpu.VMEM((2, rank // 2, cols), F32),
            pltpu.VMEM((tp, 1, cols), F32),
            pltpu.VMEM((2, rank, BLK), BF16),
            pltpu.VMEM((2, tp, rank, BLK), BF16),
            pltpu.VMEM((2, dp, rank, BLK), BF16),
            dma((5 + per,)),
            dma((tiles,)),
            dma((RING,)), dma((RING,)),
            dma((bits - 1, RING)), dma((bits - 1, RING)),
            dma((RING,)), dma((RING,)),
            dma((RING,)), dma((RING,)),
            dma((bits + 7,)), dma((bits + 7,)),
            dma((2,)), dma((2, tp)),
            dma((dp,)), dma((2, dp)),
            dma((tp,)), dma((tp,)),
        ],
        compiler_params=pltpu.CompilerParams(
            collective_id=0, has_side_effects=True, vmem_limit_bytes=LIMIT
        ),
    )(
        tokens.reshape(2, CHUNKS, ROWS, width),
        routing.T,
        weight,
        down,
        up,
        mag,
        cot.reshape(per, BLK, cols),
    )
    order = [mirrored(g, per.bit_length() - 1) for g in range(per)]
    out, ga, gb, gm = pl.pallas_call(
        functools.partial(finish, order),
        out_shape=tuple(jax.ShapeDtypeStruct(shape, kind) for shape, kind in shapes),
        in_specs=[vmem, vmem, vmem, vmem],
        out_specs=(hbm, hbm, hbm, hbm),
        scratch_shapes=[dma((per + 3,))],
    )(*(pltpu.with_memory_space_constraint(x, pltpu.VMEM) for x in held))
    return out.reshape(mine, cols), ga, gb, gm


OUT = pltpu.VMEM
LIMIT = 56 * 1024 * 1024


def solution(mesh):
    return jax.shard_map(
        functools.partial(body, mesh.shape["dp"], mesh.shape["tensor"]),
        mesh=mesh,
        in_specs=(
            P("dp", "tensor"),
            P(),
            P("tensor", "dp"),
            P(None, "tensor"),
            P(None, "dp"),
            P("dp"),
            P("tensor", "dp"),
        ),
        out_specs=(P("tensor", "dp"), P(None, "tensor"), P(None, "dp"), P("dp")),
        check_vma=False,
    )
```

```python
import functools
import math

import jax
import jax.numpy as jnp
from jax import lax
from jax.experimental import pallas as pl
from jax.experimental.pallas import tpu as pltpu
from jax.sharding import PartitionSpec as P

BLK = 128
ROWS = 16
CHUNKS = BLK // ROWS
HALVES = 4
UNITS = CHUNKS * HALVES
AHEAD = 4
LAG = 3
EARLY = 3
PAIR_LAG = 1
END_LAG = 4


def ring(lag):
    return HALVES * -(-(2 * lag + 2) // HALVES)


RING = ring(max(AHEAD - 1, LAG))
PAIR_RING = ring(PAIR_LAG)
END_RING = ring(END_LAG)
MESH = pl.DeviceIdType.MESH
F32 = jnp.float32
BF16 = jnp.bfloat16


def mirrored(value, bits):
    result = 0
    for position in range(bits):
        result = result + (value // (1 << position)) % 2 * (1 << (bits - 1 - position))
    return result


def flipped(value, bit):
    return value + bit - 2 * bit * ((value // bit) % 2)


def dots(left, right, left_dim, right_dim):
    return lax.dot_general(
        left, right, (((left_dim,), (right_dim,)), ((), ())), preferred_element_type=F32
    )


def kernel(
    cfg,
    tok_hbm, routing, w_hbm, down_hbm, up_hbm, mag_hbm, cot_hbm,
    out, ga_out, gb_out, gm_out,
    tok_in, down, up, mag, cot, w,
    raw, tok, part, near, pair, far, sq, sq_near, sq_far, factor, norm, sg,
    rp, rp_in, rgt, rg, rg_turned, proj_down, proj_turned, gm_acc,
    gb_part, gb_near, gb_sum, gb_far, gb_all, gm_in, d_loc, d_in, d_all,
    in_sem, w_sem, s0_send, s0_recv, st_send, st_recv, nr_send, nr_recv, fr_send, fr_recv,
    ms_send, ms_recv, ds_send, ds_recv, db_send, db_recv, gm_send, gm_recv,
):
    dp, tp, width, cols, rank, tile = cfg
    bits = dp.bit_length() - 1
    per = dp // tp
    tiles = cols // tile
    cut = -(-tiles // HALVES)
    pieces = [(min(p * cut, tiles), min((p + 1) * cut, tiles)) for p in range(HALVES)]
    order = [mirrored(g, per.bit_length() - 1) for g in range(per)]
    scale = 1.0 / math.sqrt(rank)
    inverse = 1.0 / math.sqrt(dp * BLK)
    high = per * ROWS
    d = lax.axis_index("dp")
    t = lax.axis_index("tensor")
    core = t % 2
    side = t // 2
    t_near, t_far = flipped(t, 1), flipped(t, 2)
    hops = [flipped(d, dp >> (k + 1)) for k in range(bits)]
    homes = (d // per, hops[0] // per)

    def copy(src, dst, send, recv, target):
        return pltpu.make_async_remote_copy(
            src_ref=src, dst_ref=dst, send_sem=send, recv_sem=recv,
            device_id=target, device_id_type=MESH,
        )

    def when(condition, action):
        pl.when(condition)(action)

    def send(make, u, *rest):
        when(u >= RING, lambda: make(u - RING, *rest).wait_send())
        make(u, *rest).start()

    def send_piece(make, c, p, size):
        back = size // HALVES
        when(c >= back, lambda: make(c - back, p).wait_send())
        make(c, p).start()

    def to_dp(k):
        return {"dp": hops[k]}

    near_id, far_id = {"tensor": t_near}, {"tensor": t_far}

    def span(p):
        return pl.ds(pieces[p][0] * tile, (pieces[p][1] - pieces[p][0]) * tile)

    def tile_at(n):
        if isinstance(n, int):
            return pl.ds(n * tile, tile)
        return pl.ds(pl.multiple_of(n * tile, tile), tile)

    def w_copy(n):
        return pltpu.make_async_copy(w_hbm.at[:, tile_at(n)], w.at[:, tile_at(n)], w_sem.at[n])

    lead = pl.ds(0, 2)
    rest = pl.ds(2, CHUNKS - 2)
    tok_lead = pltpu.make_async_copy(tok_hbm.at[:, lead], tok_in.at[:, lead], in_sem.at[0])
    tok_rest = pltpu.make_async_copy(tok_hbm.at[:, rest], tok_in.at[:, rest], in_sem.at[4 + per])
    loads = [
        pltpu.make_async_copy(down_hbm, down, in_sem.at[1]),
        pltpu.make_async_copy(up_hbm, up, in_sem.at[2]),
        pltpu.make_async_copy(mag_hbm, mag, in_sem.at[3]),
    ]
    cot_loads = [
        pltpu.make_async_copy(cot_hbm.at[g], cot.at[order[g]], in_sem.at[4 + g])
        for g in range(per)
    ]

    half = width // HALVES

    def lanes(h):
        return pl.ds(h * half, half)

    def first(u, h):
        c = u // HALVES
        return copy(
            tok_in.at[:, c, :, lanes(h)], raw.at[c, :, :, lanes(h)],
            s0_send.at[u % RING], s0_recv.at[u % RING], to_dp(0),
        )

    def stage(k, u, h, owner):
        size = 1 << k
        base = mirrored(owner, bits) // size * size
        rows = pl.ds(pl.multiple_of(base * ROWS, ROWS), size * ROWS)
        here = tok.at[u // HALVES, rows, lanes(h)]
        n = u % RING
        return copy(here, here, st_send.at[k - 1, n], st_recv.at[k - 1, n], to_dp(k))

    def near_copy(c, p):
        n = (c * HALVES + p) % PAIR_RING
        start = (1 - core) * 2
        return copy(
            part.at[c, :, pl.ds(start, 2), :, span(p)], near.at[c, :, :, :, span(p)],
            nr_send.at[n], nr_recv.at[n], near_id,
        )

    def far_copy(c, p):
        n = (c * HALVES + p) % END_RING
        return copy(
            pair.at[c, :, :, span(p)], far.at[c, :, :, span(p)],
            fr_send.at[n], fr_recv.at[n], far_id,
        )

    def home_copy(s):
        return copy(
            d_loc.at[s], d_in.at[s, t], ds_send.at[s], ds_recv.at[s, t], {"tensor": homes[s]}
        )

    def home_in(s, other):
        return copy(
            d_in.at[s, other], d_in.at[s, other], ds_send.at[s], ds_recv.at[s, other], near_id
        )

    def spread(s, k):
        return copy(
            d_all.at[s, d], d_all.at[s, d], db_send.at[k], db_recv.at[s, d], {"dp": (d + k) % dp}
        )

    def spread_in(s, source):
        return copy(
            d_all.at[s, source], d_all.at[s, source], db_send.at[0], db_recv.at[s, source],
            {"dp": hops[0]},
        )

    def gm_copy(k):
        return copy(
            gm_in.at[t], gm_in.at[t], gm_send.at[k], gm_recv.at[t], {"tensor": (t + k) % tp}
        )

    def gm_from(k):
        source = (t + k) % tp
        return copy(
            gm_in.at[source], gm_in.at[source], gm_send.at[k], gm_recv.at[source], near_id
        )

    def small(n, src, dst, target):
        return copy(src, dst, ms_send.at[n], ms_recv.at[n], target)

    sq1 = small(0, sq, sq_near, near_id)
    sq2 = small(1, sq_near, sq_far, far_id)
    rp_hops = [small(2 + k, rp.at[k], rp_in.at[k], to_dp(bits - 1 - k)) for k in range(bits)]
    n0 = 2 + bits
    rg1 = small(n0, rgt.at[t], rgt.at[t], near_id)
    rg1_in = small(n0, rgt.at[t_near], rgt.at[t_near], near_id)
    mine2 = pl.ds(side * 2, 2)
    theirs2 = pl.ds((1 - side) * 2, 2)
    rg2 = small(n0 + 1, rgt.at[mine2], rgt.at[mine2], far_id)
    rg2_in = small(n0 + 1, rgt.at[theirs2], rgt.at[theirs2], far_id)
    share = rank // 2
    gb1 = small(n0 + 2, gb_part.at[1 - core], gb_near, near_id)
    gb2 = small(n0 + 3, gb_sum, gb_far, far_id)
    gb3 = small(n0 + 4, gb_all.at[core], gb_all.at[core], near_id)
    gb3_in = small(n0 + 4, gb_all.at[1 - core], gb_all.at[1 - core], near_id)

    def each_tile(body):
        @pl.loop(0, tiles)
        def _(n):
            body(tile_at(n))

    tok_lead.start()
    barrier = pltpu.get_barrier_semaphore()

    def greet_dp(k):
        pl.semaphore_signal(barrier, inc=1, device_id={"dp": (d + k) % dp}, device_id_type=MESH)

    @pl.loop(1, dp)
    def _(k):
        greet_dp(k)

    for k in range(1, tp):
        pl.semaphore_signal(barrier, inc=1, device_id={"tensor": (t + k) % tp}, device_id_type=MESH)

    tok_rest.start()
    for load in loads:
        load.start()
    for n in range(tiles):
        w_copy(n).start()
    for load in cot_loads:
        load.start()

    gm_acc[...] = jnp.zeros_like(gm_acc)
    tok_lead.wait()
    pl.semaphore_wait(barrier, dp - 1 + tp - 1)
    for u in range(AHEAD):
        first(u, u % HALVES).start()
    tok_rest.wait()
    for load in loads:
        load.wait()

    for s in range(2):
        block = tok_in[s].reshape(BLK, width)
        d_loc[s] = dots(down[...], block, 1, 1).astype(BF16)
    for s in range(2):
        when(t != homes[s], lambda: home_copy(s).start())

    gram = dots(down[...], down[...], 1, 1)
    gram_high = gram.astype(BF16)
    gram_low = (gram - gram_high.astype(F32)).astype(BF16)

    own_live = routing[0, d] == d
    pair_live = routing[0, hops[0]] == hops[0]
    depth = 256

    def norm_tile(n):
        w_copy(n).wait()
        at = tile_at(n)
        cross = jnp.dot(down[...], w[:, at], preferred_element_type=F32)
        total = jnp.zeros((16, tile), F32)
        for r in range(0, width, depth):
            block = w[r:r + depth, at].astype(F32)
            total = total + jnp.sum((block * block).reshape(depth // 16, 16, tile), axis=0)
        ups = up[:, at]
        quad = (
            jnp.dot(gram_high, ups, preferred_element_type=F32)
            + jnp.dot(gram_low, ups, preferred_element_type=F32)
        )
        mixed = (2.0 * scale * cross + scale * scale * quad) * ups.astype(F32)
        sq[:, at] = (
            jnp.sum(total, axis=0, keepdims=True) + jnp.sum(mixed, axis=0, keepdims=True)
        )

    def gradient():
        def body(at):
            square = sq_near[:, at] + sq_far[:, at]
            size = jnp.sqrt(jnp.maximum(square, 0.25))
            ratio = mag[at].reshape(1, tile) / size
            norm[:, at] = size
            factor[:, at] = ratio
            for g in range(per):
                sg[g, :, at] = (cot[g, :, at].astype(F32) * ratio * inverse).astype(BF16)

        each_tile(body)
        for g in range(per):
            rp[0, :, g * BLK:(g + 1) * BLK] = dots(up[...], sg[g], 1, 1)

    def gather_down():
        for s in range(2):
            @pl.when(t == homes[s])
            def _():
                d_in[s, t] = d_loc[s]
                for k in range(1, tp):
                    home_in(s, (t + k) % tp).wait_recv()
                total = d_in[s, 0].astype(F32)
                for other in range(1, tp):
                    total = total + d_in[s, other].astype(F32)
                d_all[s, d] = total.astype(BF16)

                @pl.loop(1, dp)
                def _(k):
                    spread(s, k).start()

    def take_down():
        for g in range(per):
            p = t * per + g
            across = flipped(p, dp // 2)
            when(p != d, lambda: spread_in(0, p).wait_recv())
            when(across != d, lambda: spread_in(1, across).wait_recv())
            live = routing[0, p] == p
            turned = jnp.where(live, d_all[0, p], d_all[1, across])
            proj_turned[:, order[g] * BLK:(order[g] + 1) * BLK] = turned
            proj_down[order[g]] = turned.astype(F32).T.astype(BF16)

    def multiply(c, p):
        for n in range(*pieces[p]):
            at = tile_at(n)
            prod = jnp.dot(tok[c], w[:, at], preferred_element_type=F32)
            part[c, :, :, :, at] = prod.astype(BF16).reshape(per, tp, ROWS, tile)
        send_piece(near_copy, c, p, PAIR_RING)

    def combine(c, p):
        near_copy(c, p).wait_recv()
        other = core * 2 + 1 - side
        for n in range(*pieces[p]):
            at = tile_at(n)
            pair[c, :, :, at] = (
                part[c, :, other, :, at].astype(F32) + near[c, :, 1 - side, :, at].astype(F32)
            ).astype(BF16)
        send_piece(far_copy, c, p, END_RING)

    def epilogue(c, p):
        far_copy(c, p).wait_recv()
        mine = core * 2 + side
        rows = pl.ds(pl.multiple_of(c * ROWS, ROWS), ROWS)
        lhs = proj_down[:, rows, :].reshape(high, rank)
        for n in range(*pieces[p]):
            at = tile_at(n)
            total = (
                part[c, :, mine, :, at].astype(F32)
                + near[c, :, side, :, at].astype(F32)
                + far[c, :, :, at].astype(F32)
            ).reshape(high, tile)
            pre = total + scale * jnp.dot(lhs, up[:, at], preferred_element_type=F32)
            out[:, rows, at] = (pre * factor[:, at]).astype(BF16).reshape(per, ROWS, tile)
            both = cot[:, rows, at].astype(F32).reshape(high, tile) * pre
            gm_acc[:, at] += jnp.sum(both.reshape(high // 8, 8, tile), axis=0)

    def gb_start():
        for n in range(tiles):
            at = tile_at(n)
            gb_part[:, :, at] = (
                scale * jnp.dot(
                    proj_turned[...], sg[:, :, at].reshape(per * BLK, tile),
                    preferred_element_type=F32,
                )
            ).astype(BF16).reshape(2, share, tile)
        gb1.start()

    def turn_rows():
        for s in range(tp):
            turned = rgt[s].astype(F32).T.astype(BF16)
            spot = s % 2 * 2 + s // 2
            for g in range(per):
                rg[:, g, spot] = turned[g * BLK:(g + 1) * BLK].reshape(CHUNKS, ROWS, rank)
        rg_turned[...] = rg[...].reshape(dp * BLK, rank).astype(F32).T.astype(BF16)

    for n in range(min(EARLY, tiles)):
        norm_tile(n)

    later = max(0, tiles - EARLY)
    norm_last = max(1, later)
    grad_at = norm_last + 8
    gap = max(1, (UNITS - grad_at) // (bits + 1))
    ready = LAG * (bits - 1) + HALVES - 1
    steps = -(-(UNITS + ready + PAIR_LAG) // HALVES) * HALVES
    gb_at = grad_at + 4

    @pl.loop(0, steps // HALVES)
    def _(pass_):
        for h in range(HALVES):
            u = pass_ * HALVES + h

            @pl.when(u < UNITS)
            def _():
                first(u, h).wait_recv()
                c = u // HALVES
                at = lanes(h)
                own_at = pl.ds(pl.multiple_of(mirrored(d, bits) * ROWS, ROWS), ROWS)
                pair_at = pl.ds(pl.multiple_of(mirrored(hops[0], bits) * ROWS, ROWS), ROWS)
                tok[c, own_at, at] = jnp.where(own_live, tok_in[0, c, :, at], raw[c, 1, :, at])
                tok[c, pair_at, at] = jnp.where(pair_live, raw[c, 0, :, at], tok_in[1, c, :, at])
                send(functools.partial(stage, 1), u, h, d)

            when(u + AHEAD < UNITS, lambda: send(first, u + AHEAD, (h + AHEAD) % HALVES))

            for k in range(1, bits):
                v = u - LAG * k
                hv = (h - LAG * k) % HALVES

                @pl.when((v >= 0) & (v < UNITS))
                def _():
                    stage(k, v, hv, hops[k]).wait_recv()
                    if k < bits - 1:
                        send(functools.partial(stage, k + 1), v, hv, d)

            @pl.when((u >= 1) & (u <= norm_last))
            def _():
                n = EARLY + u - 1
                when(n < tiles, lambda: norm_tile(n))

            when(u == 2, gather_down)
            when(u == norm_last, lambda: sq1.start())

            @pl.when(u == norm_last + 4)
            def _():
                sq1.wait()
                sq_near[...] = sq_near[...] + sq[...]
                sq2.start()

            @pl.when(u == grad_at)
            def _():
                sq2.wait()
                for load in cot_loads:
                    load.wait()
                gradient()
                rp_hops[0].start()

            when(u == grad_at + 2, take_down)

            for k in range(bits):
                @pl.when(u == grad_at + gap * (k + 1))
                def _():
                    rp_hops[k].wait()
                    merged = rp[k] + rp_in[k]
                    if k < bits - 1:
                        rp[k + 1] = merged
                        rp_hops[k + 1].start()
                    else:
                        rgt[t] = merged.astype(BF16)
                        rg1.start()

            @pl.when(u == grad_at + gap * bits + 2)
            def _():
                rg1.wait_send()
                rg1_in.wait_recv()
                rg2.start()

            @pl.when(u == grad_at + gap * bits + 6)
            def _():
                rg2.wait_send()
                rg2_in.wait_recv()
                turn_rows()

            m = u - ready
            mq = m - PAIR_LAG
            me = mq - END_LAG
            at_m, at_q, at_e = (
                (h - ready - lag) % HALVES for lag in (0, PAIR_LAG, PAIR_LAG + END_LAG)
            )
            when((m >= 0) & (m < UNITS), lambda: multiply(m // HALVES, at_m))
            when((mq >= 0) & (mq < UNITS), lambda: combine(mq // HALVES, at_q))
            when((me >= 0) & (me < UNITS - END_LAG), lambda: epilogue(me // HALVES, at_e))

            when(u == gb_at, gb_start)

            @pl.when(u == gb_at + 3)
            def _():
                gb1.wait()
                gb_sum[...] = (gb_part[core].astype(F32) + gb_near[...].astype(F32)).astype(BF16)
                gb2.start()

            @pl.when(u == gb_at + 9)
            def _():
                gb2.wait()
                gb_all[core] = gb_sum[...].astype(F32) + gb_far[...].astype(F32)
                gb3.start()

            @pl.when(u == gb_at + 12)
            def _():
                gb3.wait_send()
                gb3_in.wait_recv()
                gb_out[...] = gb_all[...].reshape(rank, cols)

    wide = min(512, width)

    @pl.loop(0, width // wide)
    def _(n):
        at = pl.ds(pl.multiple_of(n * wide, wide), wide)
        ga_out[:, at] = scale * jnp.dot(
            rg_turned[...], tok[:, :, at].reshape(dp * BLK, wide), preferred_element_type=F32
        )

    @pl.loop(CHUNKS - RING // HALVES, CHUNKS)
    def _(c):
        for h in range(HALVES):
            u = c * HALVES + h
            first(u, h).wait_send()
            for k in range(1, bits):
                stage(k, u, h, d).wait_send()

    @pl.loop(CHUNKS - PAIR_RING // HALVES, CHUNKS)
    def _(c):
        for p in range(HALVES):
            near_copy(c, p).wait_send()

    for s in range(2):
        when(t != homes[s], lambda: home_copy(s).wait_send())

        @pl.when(t == homes[s])
        def _():
            @pl.loop(1, dp)
            def _(k):
                spread(s, k).wait_send()

    for q in range(UNITS - END_LAG, UNITS):
        epilogue(q // HALVES, q % HALVES)

    gm_in[t] = jnp.sum(gm_acc[...], axis=0, keepdims=True) / norm[...] * inverse
    for k in range(1, tp):
        gm_copy(k).start()

    @pl.loop(CHUNKS - END_RING // HALVES, CHUNKS)
    def _(c):
        for p in range(HALVES):
            far_copy(c, p).wait_send()

    for k in range(1, tp):
        gm_from(k).wait_recv()
    total = gm_in[0]
    for s in range(1, tp):
        total = total + gm_in[s]
    gm_out[...] = total.reshape(cols)
    for k in range(1, tp):
        gm_copy(k).wait_send()


def finish(order, out, ga, gb, gm, out_hbm, ga_hbm, gb_hbm, gm_hbm, sem):
    moves = [
        pltpu.make_async_copy(out.at[order[g]], out_hbm.at[g], sem.at[g])
        for g in range(len(order))
    ]
    for src, dst in ((ga, ga_hbm), (gb, gb_hbm), (gm, gm_hbm)):
        moves.append(pltpu.make_async_copy(src, dst, sem.at[len(moves)]))
    for move in moves:
        move.start()
    for move in moves:
        move.wait()


def body(dp, tp, tokens, routing, weight, down, up, mag, cot):
    width, cols = weight.shape
    rank = down.shape[0]
    per = dp // tp
    bits = dp.bit_length() - 1
    tile = next(size for size in (512, 256, 128) if cols % size == 0)
    tiles = cols // tile
    cfg = (dp, tp, width, cols, rank, tile)
    vmem = pl.BlockSpec(memory_space=pltpu.VMEM)
    hbm = pl.BlockSpec(memory_space=pltpu.HBM)
    dma = pltpu.SemaphoreType.DMA
    mine = per * BLK
    shapes = (
        ((per, BLK, cols), BF16),
        ((rank, width), F32),
        ((rank, cols), F32),
        ((cols,), F32),
    )
    held = pl.pallas_call(
        functools.partial(kernel, cfg),
        out_shape=tuple(OUT(shape, kind) for shape, kind in shapes),
        in_specs=[hbm, pl.BlockSpec(memory_space=pltpu.SMEM), hbm, hbm, hbm, hbm, hbm],
        out_specs=(vmem, vmem, vmem, vmem),
        scratch_shapes=[
            pltpu.VMEM((2, CHUNKS, ROWS, width), BF16),
            pltpu.VMEM((rank, width), BF16),
            pltpu.VMEM((rank, cols), BF16),
            pltpu.VMEM((cols,), F32),
            pltpu.VMEM((per, BLK, cols), BF16),
            pltpu.VMEM((width, cols), BF16),
            pltpu.VMEM((CHUNKS, 2, ROWS, width), BF16),
            pltpu.VMEM((CHUNKS, dp * ROWS, width), BF16),
            pltpu.VMEM((CHUNKS, per, tp, ROWS, cols), BF16),
            pltpu.VMEM((CHUNKS, per, 2, ROWS, cols), BF16),
            pltpu.VMEM((CHUNKS, per, ROWS, cols), BF16),
            pltpu.VMEM((CHUNKS, per, ROWS, cols), BF16),
            pltpu.VMEM((1, cols), F32),
            pltpu.VMEM((1, cols), F32),
            pltpu.VMEM((1, cols), F32),
            pltpu.VMEM((1, cols), F32),
            pltpu.VMEM((1, cols), F32),
            pltpu.VMEM((per, BLK, cols), BF16),
            pltpu.VMEM((bits, rank, mine), F32),
            pltpu.VMEM((bits, rank, mine), F32),
            pltpu.VMEM((tp, rank, mine), BF16),
            pltpu.VMEM((CHUNKS, per, tp, ROWS, rank), BF16),
            pltpu.VMEM((rank, dp * BLK), BF16),
            pltpu.VMEM((per, BLK, rank), BF16),
            pltpu.VMEM((rank, mine), BF16),
            pltpu.VMEM((8, cols), F32),
            pltpu.VMEM((2, rank // 2, cols), BF16),
            pltpu.VMEM((rank // 2, cols), BF16),
            pltpu.VMEM((rank // 2, cols), BF16),
            pltpu.VMEM((rank // 2, cols), BF16),
            pltpu.VMEM((2, rank // 2, cols), F32),
            pltpu.VMEM((tp, 1, cols), F32),
            pltpu.VMEM((2, rank, BLK), BF16),
            pltpu.VMEM((2, tp, rank, BLK), BF16),
            pltpu.VMEM((2, dp, rank, BLK), BF16),
            dma((5 + per,)),
            dma((tiles,)),
            dma((RING,)), dma((RING,)),
            dma((bits - 1, RING)), dma((bits - 1, RING)),
            dma((PAIR_RING,)), dma((PAIR_RING,)),
            dma((END_RING,)), dma((END_RING,)),
            dma((bits + 7,)), dma((bits + 7,)),
            dma((2,)), dma((2, tp)),
            dma((dp,)), dma((2, dp)),
            dma((tp,)), dma((tp,)),
        ],
        compiler_params=pltpu.CompilerParams(
            collective_id=0, has_side_effects=True, vmem_limit_bytes=LIMIT
        ),
    )(
        tokens.reshape(2, CHUNKS, ROWS, width),
        routing.T,
        weight,
        down,
        up,
        mag,
        cot.reshape(per, BLK, cols),
    )
    order = [mirrored(g, per.bit_length() - 1) for g in range(per)]
    out, ga, gb, gm = pl.pallas_call(
        functools.partial(finish, order),
        out_shape=tuple(jax.ShapeDtypeStruct(shape, kind) for shape, kind in shapes),
        in_specs=[vmem, vmem, vmem, vmem],
        out_specs=(hbm, hbm, hbm, hbm),
        scratch_shapes=[dma((per + 3,))],
    )(*(pltpu.with_memory_space_constraint(x, pltpu.VMEM) for x in held))
    return out.reshape(mine, cols), ga, gb, gm


OUT = pltpu.VMEM
LIMIT = 56 * 1024 * 1024


def solution(mesh):
    return jax.shard_map(
        functools.partial(body, mesh.shape["dp"], mesh.shape["tensor"]),
        mesh=mesh,
        in_specs=(
            P("dp", "tensor"),
            P(),
            P("tensor", "dp"),
            P(None, "tensor"),
            P(None, "dp"),
            P("dp"),
            P("tensor", "dp"),
        ),
        out_specs=(P("tensor", "dp"), P(None, "tensor"), P(None, "dp"), P("dp")),
        check_vma=False,
    )
```
